32 devices in a mesh: sp: 16 (over z, x, core), dp: 2 (over y).
Axes of the slice: x: 2, y: 2, z: 4, core: 2. Of those that a mesh axis runs over, the one named last changes fastest.
Arguments:
- queries: bfloat16 [1536, 24, 128], P(('dp', 'sp')), parts along dimension 0, may hold values from -12 to 12
- keys: bfloat16 [1536, 24, 128], P(('dp', 'sp')), parts along dimension 0, may hold values from -6 to 6
- values: bfloat16 [1536, 24, 128], P(('dp', 'sp')), parts along dimension 0, may hold values from -6 to 6
Outputs:
- attended: bfloat16 [1536, 3072], P(('dp', 'sp')), parts along dimension 0
The draws below stay inside these ranges and needn't reach their ends.
There are 2 independent parts, one for each index of `dp`. The reference program is written for one: setup_inputs(seed, part) draws one part's arguments, and reference() takes and returns one part's arrays. A program takes and returns all parts, laid end to end along the dimension named above; each array names one. Nothing has to cross between parts.
All inputs are finite; a program needn't handle non-finite values.
Results may differ from the reference program's by a relative error of at most 0.0049.
Values may be sent and summed in bfloat16 or wider, within the bound.
No kernel may reach another device: no remote copies, remote signals or barrier semaphores. Data moves between devices by JAX's collectives and lax.ppermute only.
A program may use at most 64 MiB of HBM per device.

```python
import jax
import jax.numpy as jnp
from jax import lax

HEADS = 24
HEAD_DIM = 128
SEQ = 768


def draw_queries(key, part):
    own_key = jax.random.fold_in(key, 1)
    result = 2.5 * jax.random.truncated_normal(own_key, -4.8, 4.8, (SEQ, HEADS, HEAD_DIM), jnp.float32)
    return result.astype(jnp.bfloat16)


def draw_keys(key, part):
    own_key = jax.random.fold_in(key, 2)
    result = jax.random.truncated_normal(own_key, -6.0, 6.0, (SEQ, HEADS, HEAD_DIM), jnp.float32)
    return result.astype(jnp.bfloat16)


def levels(rng, extent, pieces, least, largest):
    level, own = 1.0, jax.random.fold_in(rng, 6)
    for position, shards_of in pieces:
        steps = jnp.exp(jax.random.uniform(jax.random.fold_in(own, position), (shards_of,), jnp.float32, least / len(pieces), largest / len(pieces)))
        level = level * jnp.repeat(steps, extent[position] // shards_of).reshape([-1 if axis == position else 1 for axis in range(len(extent))])
    return level


def gaussian(stream_key, shape, scale, bound, pieces=(), dtype=jnp.bfloat16):
    drawn = jax.random.normal(stream_key, shape, jnp.float32) * scale
    if len(pieces) > 0:
        drawn = levels(stream_key, shape, pieces, -0.22, 0.18) * drawn
    return jnp.clip(drawn, min=-bound, max=bound).astype(dtype)


def setup_inputs(seed: int = 0, part: int = 0) -> dict:
    splits = jax.random.split(jax.random.key(seed), 4)
    part_keys = jax.random.split(jax.random.fold_in(splits[3], part), 4)
    return {
        "queries": draw_queries(jax.random.fold_in(jax.random.fold_in(splits[3], part), 71), part),
        "keys": draw_keys(jax.random.fold_in(jax.random.fold_in(splits[3], part), 71), part),
        "values": gaussian(part_keys[2], (SEQ, HEADS, HEAD_DIM), 1.0, 6.0, ((0, 16),)),
    }


def attend(triple):
    head_q, head_k, head_v = triple
    scale = 1.0 / (head_q.shape[-1] ** 0.5)
    scores = jnp.dot(head_q, head_k.T, preferred_element_type=jnp.float32) * scale
    weights = jax.nn.softmax(scores, axis=-1).astype(jnp.bfloat16)
    return jnp.dot(weights, head_v, preferred_element_type=jnp.float32)


def reference(queries, keys, values):
    seq_len, heads, width = queries.shape
    result = lax.map(attend, (queries.transpose(1, 0, 2), keys.transpose(1, 0, 2), values.transpose(1, 0, 2)))
    return result.transpose(1, 0, 2).reshape(seq_len, heads * width).astype(jnp.bfloat16)
```

```python
import functools

import jax
import jax.numpy as jnp
from jax import lax
from jax.experimental import pallas as pl
from jax.experimental.pallas import tpu as pltpu
from jax.sharding import PartitionSpec as P


VMEM = pltpu.MemorySpace.VMEM
SMEM = pltpu.MemorySpace.SMEM


def pack_kernel(group_ref, q_ref, k_ref, v_ref, *refs, groups, per_group):
    outs, wide = refs[:groups], refs[groups]
    tokens, heads, width = q_ref.shape
    group = group_ref[0]
    for part, ref in enumerate((q_ref, k_ref, v_ref)):
        wide[part] = ref[...].reshape(tokens * heads, width).astype(jnp.float32)
        for mask in range(groups):
            first = (group ^ mask) * per_group
            for head in range(per_group):
                rows = wide[part, pl.ds(first + head, tokens, stride=heads), :]
                outs[mask][part, head] = rows.astype(jnp.bfloat16)


def pack(group, queries, keys, values, groups):
    tokens, heads, width = queries.shape
    per_group = heads // groups
    piece = jax.ShapeDtypeStruct((3, per_group, tokens, width), queries.dtype)
    return pl.pallas_call(
        functools.partial(pack_kernel, groups=groups, per_group=per_group),
        in_specs=[pl.BlockSpec(memory_space=SMEM)] + [pl.BlockSpec(memory_space=VMEM)] * 3,
        out_specs=[pl.BlockSpec(memory_space=VMEM)] * groups,
        out_shape=[piece] * groups,
        scratch_shapes=[pltpu.VMEM((3, tokens * heads, width), jnp.float32)],
    )(group, queries, keys, values)


def attend_kernel(*refs, groups, blocks):
    count = groups * blocks
    pieces, outs = refs[:count], refs[count : count + groups]
    head_q, head_k, head_v = refs[count + groups :]
    per_group, tokens, width = pieces[0].shape[1:]
    scale = 1.0 / width**0.5
    for head in range(per_group):
        for index, piece in enumerate(pieces):
            rows = pl.ds(index * tokens, tokens)
            if index < groups:
                head_q[head, rows, :] = piece[0, head]
            head_k[head, rows, :] = piece[1, head]
            head_v[head, rows, :] = piece[2, head]
        scores = lax.dot_general(head_q[head], head_k[head], (((1,), (1,)), ((), ())), preferred_element_type=jnp.float32)
        scores = scores * scale
        weights = jnp.exp(scores - jnp.max(scores, axis=-1, keepdims=True))
        weights = weights * (1.0 / jnp.sum(weights, axis=-1, keepdims=True))
        result = jnp.dot(weights.astype(jnp.bfloat16), head_v[head], preferred_element_type=jnp.float32)
        result = result.astype(jnp.bfloat16)
        for mask in range(groups):
            outs[mask][:, head * width : (head + 1) * width] = result[mask * tokens : (mask + 1) * tokens]


def attend(pieces, groups, blocks):
    _, per_group, tokens, width = pieces[0].shape
    out = jax.ShapeDtypeStruct((tokens, per_group * width), pieces[0].dtype)
    return pl.pallas_call(
        functools.partial(attend_kernel, groups=groups, blocks=blocks),
        in_specs=[pl.BlockSpec(memory_space=VMEM)] * len(pieces),
        out_specs=[pl.BlockSpec(memory_space=VMEM)] * groups,
        out_shape=[out] * groups,
        scratch_shapes=[
            pltpu.VMEM((per_group, groups * tokens, width), pieces[0].dtype),
            pltpu.VMEM((per_group, groups * blocks * tokens, width), pieces[0].dtype),
            pltpu.VMEM((per_group, groups * blocks * tokens, width), pieces[0].dtype),
        ],
    )(*pieces)


def unpack_kernel(group_ref, *refs):
    pieces, out_ref = refs[:-1], refs[-1]
    feat = pieces[0].shape[1]
    group = group_ref[0]
    for mask, piece in enumerate(pieces):
        first = pl.multiple_of((group ^ mask) * feat, 128)
        out_ref[:, pl.ds(first, feat)] = piece[...]


def unpack(group, pieces):
    tokens, feat = pieces[0].shape
    return pl.pallas_call(
        unpack_kernel,
        in_specs=[pl.BlockSpec(memory_space=SMEM)] + [pl.BlockSpec(memory_space=VMEM)] * len(pieces),
        out_specs=pl.BlockSpec(memory_space=VMEM),
        out_shape=jax.ShapeDtypeStruct((tokens, len(pieces) * feat), pieces[0].dtype),
    )(group, *pieces)


def shards(queries, keys, values):
    heads = queries.shape[1]
    devices = lax.axis_size("sp")
    groups = min(heads & -heads, devices & -devices)
    blocks = devices // groups
    group = (lax.axis_index("sp") // blocks).astype(jnp.int32).reshape(1)

    def across(piece, mask):
        if mask == 0:
            return piece
        pairs = [(i, (i // blocks ^ mask) * blocks + i % blocks) for i in range(devices)]
        return lax.ppermute(piece, "sp", pairs)

    def within(piece, step):
        pairs = [(i, i // blocks * blocks + (i + step) % blocks) for i in range(devices)]
        return lax.ppermute(piece, "sp", pairs)

    sent = pack(group, queries, keys, values, groups)
    own = [across(piece, mask) for mask, piece in enumerate(sent)]
    others = [within(piece, step) for step in range(1, blocks) for piece in own]
    results = attend(own + others, groups, blocks)
    returned = [across(piece, mask) for mask, piece in enumerate(results)]
    return unpack(group, returned)


def solution(mesh):
    spec = P(("dp", "sp"), None, None)
    return jax.shard_map(
        shards,
        mesh=mesh,
        in_specs=(spec, spec, spec),
        out_specs=P(("dp", "sp"), None),
        check_vma=False,
    )
```

```python
import functools
import math

import jax
import jax.numpy as jnp
from jax import lax
from jax.experimental import pallas as pl
from jax.experimental.pallas import tpu as pltpu
from jax.sharding import PartitionSpec as P


CORES = 2
GROUPS = 4

VMEM = pltpu.MemorySpace.VMEM
SMEM = pltpu.MemorySpace.SMEM


def local(count):
    return [pl.BlockSpec(memory_space=VMEM)] * count


def scalar():
    return [pl.BlockSpec(memory_space=SMEM)]


def pack_kernel(group_ref, q_ref, k_ref, v_ref, *refs, groups):
    near, far, wide = refs[:groups], refs[groups : 2 * groups], refs[2 * groups]
    tokens, heads, width = q_ref.shape
    per_group = heads // groups
    group = group_ref[0]
    for part, ref in enumerate((k_ref, v_ref, q_ref)):
        wide[part] = ref[...].reshape(tokens * heads, width).astype(jnp.float32)
        for mask in range(groups):
            first = (group ^ mask) * per_group
            for head in range(per_group):
                rows = wide[part, pl.ds(first + head, tokens, stride=heads), :].astype(q_ref.dtype)
                near[mask][part, head] = rows
                if part < 2:
                    far[mask][part, head] = rows


def pack(group, queries, keys, values, groups):
    tokens, heads, width = queries.shape
    near = OUT((3, heads // groups, tokens, width), queries.dtype)
    far = OUT((2, heads // groups, tokens, width), queries.dtype)
    outs = pl.pallas_call(
        functools.partial(pack_kernel, groups=groups),
        in_specs=scalar() + local(3),
        out_specs=local(2 * groups),
        out_shape=[near] * groups + [far] * groups,
        scratch_shapes=[pltpu.VMEM((3, tokens * heads, width), jnp.float32)],
    )(group, queries, keys, values)
    return outs[:groups], outs[groups:]


def block(head_q, pieces, head, scale):
    head_k = jnp.concatenate([piece[0, head] for piece in pieces])
    head_v = jnp.concatenate([piece[1, head] for piece in pieces])
    scores = lax.dot_general(head_q, head_k, (((1,), (1,)), ((), ())), preferred_element_type=jnp.float32)
    largest = jnp.max(scores, axis=-1, keepdims=True)
    weights = jnp.exp2((scores - largest) * scale)
    total = jnp.sum(weights, axis=-1, keepdims=True)
    summed = jnp.dot(weights.astype(head_v.dtype), head_v, preferred_element_type=jnp.float32)
    return largest, total, summed


def first_kernel(*refs, groups, count, scale):
    pieces, (q_out, largest_out, total_out, summed_out) = refs[:count], refs[count:]
    for head in range(q_out.shape[0]):
        head_q = jnp.concatenate([piece[2, head] for piece in pieces[:groups]])
        q_out[head] = head_q
        largest, total, summed = block(head_q, pieces, head, scale)
        largest_out[head] = largest
        total_out[head] = total
        summed_out[head] = summed


def attend_first(pieces, groups, scale):
    _, per_group, tokens, width = pieces[0].shape
    rows = groups * tokens
    return pl.pallas_call(
        functools.partial(first_kernel, groups=groups, count=len(pieces), scale=scale),
        in_specs=local(len(pieces)),
        out_specs=local(4),
        out_shape=[
            OUT((per_group, rows, width), pieces[0].dtype),
            OUT((per_group, rows, 1), jnp.float32),
            OUT((per_group, rows, 1), jnp.float32),
            OUT((per_group, rows, width), jnp.float32),
        ],
    )(*pieces)


def last_kernel(q_ref, largest_ref, total_ref, summed_ref, *refs, count, scale):
    pieces, outs = refs[:count], refs[count:]
    per_group, tokens, width = pieces[0].shape[1:]
    for head in range(per_group):
        largest, total, summed = block(q_ref[head], pieces, head, scale)
        before = largest_ref[head]
        top = jnp.maximum(largest, before)
        now, then = jnp.exp2((largest - top) * scale), jnp.exp2((before - top) * scale)
        inverse = 1.0 / (total * now + total_ref[head] * then)
        result = summed * (now * inverse) + summed_ref[head] * (then * inverse)
        result = result.astype(pieces[0].dtype)
        for mask, out in enumerate(outs):
            out[:, head * width : (head + 1) * width] = result[mask * tokens : (mask + 1) * tokens]


def attend_last(state, pieces, groups, scale):
    _, per_group, tokens, width = pieces[0].shape
    out = OUT((tokens, per_group * width), pieces[0].dtype)
    return pl.pallas_call(
        functools.partial(last_kernel, count=len(pieces), scale=scale),
        in_specs=local(4 + len(pieces)),
        out_specs=local(groups),
        out_shape=[out] * groups,
    )(*state, *pieces)


def unpack_kernel(group_ref, *refs):
    pieces, out_ref = refs[:-1], refs[-1]
    feat = pieces[0].shape[1]
    group = group_ref[0]
    for mask, piece in enumerate(pieces):
        first = pl.multiple_of((group ^ mask) * feat, 128)
        out_ref[:, pl.ds(first, feat)] = piece[...]


def unpack(group, pieces):
    tokens, feat = pieces[0].shape
    return pl.pallas_call(
        unpack_kernel,
        in_specs=scalar() + local(len(pieces)),
        out_specs=pl.BlockSpec(memory_space=VMEM),
        out_shape=jax.ShapeDtypeStruct((tokens, len(pieces) * feat), pieces[0].dtype),
    )(group, *pieces)


def OUT(shape, dtype):
    return OUTF(shape, dtype)

OUTF = jax.ShapeDtypeStruct


def shards(queries, keys, values):
    heads, width = queries.shape[1:]
    devices = lax.axis_size("sp")
    groups = min(GROUPS, heads & -heads, devices // CORES)
    regions = devices // (groups * CORES)
    scale = math.log2(math.e) / math.sqrt(width)
    group = (lax.axis_index("sp") // CORES % groups).astype(jnp.int32).reshape(1)

    def across(piece, mask, step):
        pairs = []
        for i in range(devices):
            region, own, core = i // (groups * CORES), i // CORES % groups, i % CORES
            pairs.append((i, (((region + step) % regions) * groups + (own ^ mask)) * CORES + core))
        return lax.ppermute(piece, "sp", pairs)

    def sibling(piece):
        pairs = [(i, i // CORES * CORES + (i + 1) % CORES) for i in range(devices)]
        return lax.ppermute(piece, "sp", pairs)

    near, far = pack(group, queries, keys, values, groups)
    order = list(range(groups))[::-1]
    far_in = [across(far[mask], mask, step) for step in range(1, regions) for mask in order]
    near_in = [near[0]] + [across(near[mask], mask, 0) for mask in range(1, groups)]
    near_all = near_in + [sibling(far[0])] + [sibling(piece) for piece in near_in[1:]]
    state = attend_first(near_all, groups, scale)
    far_all = far_in + [sibling(piece) for piece in far_in]
    results = attend_last(state, far_all, groups, scale)
    returned = [results[0]] + [across(results[mask], mask, 0) for mask in range(1, groups)]
    return unpack(group, returned)


def solution(mesh):
    spec = P(("dp", "sp"), None, None)
    return jax.shard_map(
        shards,
        mesh=mesh,
        in_specs=(spec, spec, spec),
        out_specs=P(("dp", "sp"), None),
        check_vma=False,
    )
```

```python
import functools
import math

import jax
import jax.numpy as jnp
from jax import lax
from jax.experimental import pallas as pl
from jax.experimental.pallas import tpu as pltpu
from jax.sharding import PartitionSpec as P


CORES = 2
GROUPS = 4

VMEM = pltpu.MemorySpace.VMEM
SMEM = pltpu.MemorySpace.SMEM
PARAMS = pltpu.CompilerParams(vmem_limit_bytes=24 << 20)


def local(count):
    return [pl.BlockSpec(memory_space=VMEM)] * count


def scalar():
    return [pl.BlockSpec(memory_space=SMEM)]


def pack_kernel(group_ref, q_ref, k_ref, v_ref, *refs, groups):
    near, far, wide = refs[:groups], refs[groups : 2 * groups], refs[2 * groups]
    tokens, heads, width = q_ref.shape
    per_group = heads // groups
    group = group_ref[0]
    for part, ref in enumerate((k_ref, v_ref, q_ref)):
        wide[part] = ref[...].reshape(tokens * heads, width).astype(jnp.float32)
        for mask in range(groups):
            first = (group ^ mask) * per_group
            for head in range(per_group):
                rows = wide[part, pl.ds(first + head, tokens, stride=heads), :].astype(q_ref.dtype)
                near[mask][part, head] = rows
                if part < 2:
                    far[mask][part, head] = rows


def pack(group, queries, keys, values, groups):
    tokens, heads, width = queries.shape
    near = pltpu.VMEM((3, heads // groups, tokens, width), queries.dtype)
    far = pltpu.VMEM((2, heads // groups, tokens, width), queries.dtype)
    outs = pl.pallas_call(
        functools.partial(pack_kernel, groups=groups),
        in_specs=scalar() + local(3),
        out_specs=local(2 * groups),
        out_shape=[near] * groups + [far] * groups,
        scratch_shapes=[pltpu.VMEM((3, tokens * heads, width), jnp.float32)],
        compiler_params=PARAMS,
    )(group, queries, keys, values)
    return outs[:groups], outs[groups:]


def block(head_q, pieces, head, scale):
    head_k = jnp.concatenate([piece[0, head] for piece in pieces])
    head_v = jnp.concatenate([piece[1, head] for piece in pieces])
    scores = lax.dot_general(head_q, head_k, (((1,), (1,)), ((), ())), preferred_element_type=jnp.float32)
    largest = jnp.max(scores, axis=-1, keepdims=True)
    weights = jnp.exp2((scores - largest) * scale)
    total = jnp.sum(weights, axis=-1, keepdims=True)
    summed = jnp.dot(weights.astype(head_v.dtype), head_v, preferred_element_type=jnp.float32)
    return largest, total, summed


def first_kernel(*refs, groups, count, scale):
    pieces, (q_out, largest_out, total_out, summed_out) = refs[:count], refs[count:]
    for head in range(q_out.shape[0]):
        head_q = jnp.concatenate([piece[2, head] for piece in pieces[:groups]])
        q_out[head] = head_q
        largest, total, summed = block(head_q, pieces, head, scale)
        largest_out[head] = largest
        total_out[head] = total
        summed_out[head] = summed


def attend_first(pieces, groups, scale):
    _, per_group, tokens, width = pieces[0].shape
    rows = groups * tokens
    return pl.pallas_call(
        functools.partial(first_kernel, groups=groups, count=len(pieces), scale=scale),
        in_specs=local(len(pieces)),
        out_specs=local(4),
        out_shape=[
            pltpu.VMEM((per_group, rows, width), pieces[0].dtype),
            pltpu.VMEM((per_group, rows, 1), jnp.float32),
            pltpu.VMEM((per_group, rows, 1), jnp.float32),
            pltpu.VMEM((per_group, rows, width), jnp.float32),
        ],
        compiler_params=PARAMS,
    )(*map(inside, pieces))


def last_kernel(q_ref, largest_ref, total_ref, summed_ref, *refs, count, scale):
    pieces, outs = refs[:count], refs[count:]
    per_group, tokens, width = pieces[0].shape[1:]
    for head in range(per_group):
        largest, total, summed = block(q_ref[head], pieces, head, scale)
        before = largest_ref[head]
        top = jnp.maximum(largest, before)
        now, then = jnp.exp2((largest - top) * scale), jnp.exp2((before - top) * scale)
        inverse = 1.0 / (total * now + total_ref[head] * then)
        result = summed * (now * inverse) + summed_ref[head] * (then * inverse)
        result = result.astype(pieces[0].dtype)
        for mask, out in enumerate(outs):
            out[:, head * width : (head + 1) * width] = result[mask * tokens : (mask + 1) * tokens]


def attend_last(state, pieces, groups, scale):
    _, per_group, tokens, width = pieces[0].shape
    out = pltpu.VMEM((tokens, per_group * width), pieces[0].dtype)
    return pl.pallas_call(
        functools.partial(last_kernel, count=len(pieces), scale=scale),
        in_specs=local(4 + len(pieces)),
        out_specs=local(groups),
        out_shape=[out] * groups,
        compiler_params=PARAMS,
    )(*map(inside, state), *map(inside, pieces))


def unpack_kernel(group_ref, *refs):
    pieces, out_ref = refs[:-1], refs[-1]
    feat = pieces[0].shape[1]
    group = group_ref[0]
    for mask, piece in enumerate(pieces):
        first = pl.multiple_of((group ^ mask) * feat, 128)
        out_ref[:, pl.ds(first, feat)] = piece[...]


def unpack(group, pieces):
    tokens, feat = pieces[0].shape
    return pl.pallas_call(
        unpack_kernel,
        in_specs=scalar() + local(len(pieces)),
        out_specs=pl.BlockSpec(memory_space=VMEM),
        out_shape=jax.ShapeDtypeStruct((tokens, len(pieces) * feat), pieces[0].dtype),
        compiler_params=PARAMS,
    )(group, *map(inside, pieces))


def inside(x):
    return pltpu.with_memory_space_constraint(x, pltpu.MemorySpace.VMEM)


def shards(queries, keys, values):
    heads, width = queries.shape[1:]
    devices = lax.axis_size("sp")
    groups = min(GROUPS, heads & -heads, devices // CORES)
    regions = devices // (groups * CORES)
    scale = math.log2(math.e) / math.sqrt(width)
    group = (lax.axis_index("sp") // CORES % groups).astype(jnp.int32).reshape(1)

    def across(piece, mask, step):
        pairs = []
        for i in range(devices):
            region, own, core = i // (groups * CORES), i // CORES % groups, i % CORES
            pairs.append((i, (((region + step) % regions) * groups + (own ^ mask)) * CORES + core))
        return lax.ppermute(piece, "sp", pairs)

    def sibling(piece):
        pairs = [(i, i // CORES * CORES + (i + 1) % CORES) for i in range(devices)]
        return lax.ppermute(piece, "sp", pairs)

    near, far = pack(group, queries, keys, values, groups)
    far_in, far_all, near_in, near_all = [], [], [near[0]], []
    for step in range(1, regions):
        for mask in reversed(range(groups)):
            far_in.append(across(far[mask], mask, step))
    for mask in range(1, groups):
        near_in.append(across(near[mask], mask, 0))
    near_all = near_in + [sibling(far[0])] + [sibling(piece) for piece in near_in[1:]]
    state = attend_first(near_all, groups, scale)
    far_all = far_in + [sibling(piece) for piece in far_in]
    results = attend_last(state, far_all, groups, scale)
    returned = [results[0]] + [across(results[mask], mask, 0) for mask in range(1, groups)]
    return unpack(group, returned)


def solution(mesh):
    spec = P(("dp", "sp"), None, None)
    return jax.shard_map(
        shards,
        mesh=mesh,
        in_specs=(spec, spec, spec),
        out_specs=P(("dp", "sp"), None),
        check_vma=False,
    )
```

```python
import functools
import math

import jax
import jax.numpy as jnp
from jax import lax
from jax.experimental import pallas as pl
from jax.experimental.pallas import tpu as pltpu
from jax.sharding import PartitionSpec as P


CORES = 2
GROUPS = 4

VMEM = pltpu.MemorySpace.VMEM
SMEM = pltpu.MemorySpace.SMEM
PARAMS = pltpu.CompilerParams(vmem_limit_bytes=24 << 20)


def local(count):
    return [pl.BlockSpec(memory_space=VMEM)] * count


def scalar():
    return [pl.BlockSpec(memory_space=SMEM)]


def pack_kernel(group_ref, q_ref, k_ref, v_ref, *refs, groups):
    near, far = refs[:groups], refs[groups : 2 * groups]
    landed, wide, arrived = refs[2 * groups :]
    tokens, heads, width = q_ref.shape
    per_group = heads // groups
    group = group_ref[0]
    copies = []
    for part, ref in enumerate((k_ref, v_ref, q_ref)):
        copies.append(pltpu.make_async_copy(ref, landed.at[part], arrived.at[part]))
        copies[part].start()
    for part in range(3):
        copies[part].wait()
        wide[part] = landed[part].reshape(tokens * heads, width).astype(jnp.float32)
        for mask in range(groups):
            first = (group ^ mask) * per_group
            for head in range(per_group):
                rows = wide[part, pl.ds(first + head, tokens, stride=heads), :].astype(q_ref.dtype)
                near[mask][part, head] = rows
                if part < 2:
                    far[mask][part, head] = rows


def pack(group, queries, keys, values, groups):
    tokens, heads, width = queries.shape
    near = pltpu.VMEM((3, heads // groups, tokens, width), queries.dtype)
    far = pltpu.VMEM((2, heads // groups, tokens, width), queries.dtype)
    outs = pl.pallas_call(
        functools.partial(pack_kernel, groups=groups),
        in_specs=scalar() + [pl.BlockSpec(memory_space=pltpu.MemorySpace.HBM)] * 3,
        out_specs=local(2 * groups),
        out_shape=[near] * groups + [far] * groups,
        scratch_shapes=[
            pltpu.VMEM((3, tokens, heads, width), queries.dtype),
            pltpu.VMEM((3, tokens * heads, width), jnp.float32),
            pltpu.SemaphoreType.DMA((3,)),
        ],
        compiler_params=PARAMS,
    )(group, *(pltpu.with_memory_space_constraint(x, pltpu.MemorySpace.HBM) for x in (queries, keys, values)))
    return outs[:groups], outs[groups:]


def block(head_q, pieces, head, scale):
    head_k = jnp.concatenate([piece[0, head] for piece in pieces])
    head_v = jnp.concatenate([piece[1, head] for piece in pieces])
    scores = lax.dot_general(head_q, head_k, (((1,), (1,)), ((), ())), preferred_element_type=jnp.float32)
    largest = jnp.max(scores, axis=-1, keepdims=True)
    weights = jnp.exp2((scores - largest) * scale)
    total = jnp.sum(weights, axis=-1, keepdims=True)
    summed = jnp.dot(weights.astype(head_v.dtype), head_v, preferred_element_type=jnp.float32)
    return largest, total, summed


def first_kernel(*refs, groups, count, scale):
    pieces, (q_out, largest_out, total_out, summed_out) = refs[:count], refs[count:]
    for head in range(q_out.shape[0]):
        head_q = jnp.concatenate([piece[2, head] for piece in pieces[:groups]])
        q_out[head] = head_q
        largest, total, summed = block(head_q, pieces, head, scale)
        largest_out[head] = largest
        total_out[head] = total
        summed_out[head] = summed


def attend_first(pieces, groups, scale):
    _, per_group, tokens, width = pieces[0].shape
    rows = groups * tokens
    return pl.pallas_call(
        functools.partial(first_kernel, groups=groups, count=len(pieces), scale=scale),
        in_specs=local(len(pieces)),
        out_specs=local(4),
        out_shape=[
            pltpu.VMEM((per_group, rows, width), pieces[0].dtype),
            pltpu.VMEM((per_group, rows, 1), jnp.float32),
            pltpu.VMEM((per_group, rows, 1), jnp.float32),
            pltpu.VMEM((per_group, rows, width), jnp.float32),
        ],
        compiler_params=PARAMS,
    )(*map(inside, pieces))


def merge(refs, pieces, head, scale):
    q_ref, largest_ref, total_ref, summed_ref = refs
    largest, total, summed = block(q_ref[head], pieces, head, scale)
    before = largest_ref[head]
    top = jnp.maximum(largest, before)
    now, then = jnp.exp2((largest - top) * scale), jnp.exp2((before - top) * scale)
    return top, now, then, total * now + total_ref[head] * then, summed, summed_ref[head]


def middle_kernel(*refs, count, scale):
    state, pieces, (largest_out, total_out, summed_out) = refs[:4], refs[4 : 4 + count], refs[4 + count :]
    for head in range(pieces[0].shape[1]):
        top, now, then, total, summed, earlier = merge(state, pieces, head, scale)
        largest_out[head] = top
        total_out[head] = total
        summed_out[head] = summed * now + earlier * then


def attend_middle(state, pieces, scale):
    shapes = [pltpu.VMEM(part.shape, part.dtype) for part in state[1:]]
    outs = pl.pallas_call(
        functools.partial(middle_kernel, count=len(pieces), scale=scale),
        in_specs=local(4 + len(pieces)),
        out_specs=local(3),
        out_shape=shapes,
        compiler_params=PARAMS,
    )(*map(inside, state), *map(inside, pieces))
    return [state[0]] + list(outs)


def last_kernel(*refs, count, scale):
    state, pieces, outs = refs[:4], refs[4 : 4 + count], refs[4 + count :]
    per_group, tokens, width = pieces[0].shape[1:]
    for head in range(per_group):
        _, now, then, total, summed, earlier = merge(state, pieces, head, scale)
        inverse = 1.0 / total
        result = summed * (now * inverse) + earlier * (then * inverse)
        result = result.astype(pieces[0].dtype)
        for mask, out in enumerate(outs):
            out[:, head * width : (head + 1) * width] = result[mask * tokens : (mask + 1) * tokens]


def attend_last(state, pieces, groups, scale):
    _, per_group, tokens, width = pieces[0].shape
    out = pltpu.VMEM((tokens, per_group * width), pieces[0].dtype)
    return pl.pallas_call(
        functools.partial(last_kernel, count=len(pieces), scale=scale),
        in_specs=local(4 + len(pieces)),
        out_specs=local(groups),
        out_shape=[out] * groups,
        compiler_params=PARAMS,
    )(*map(inside, state), *map(inside, pieces))


def unpack_kernel(group_ref, *refs):
    pieces, out_ref = refs[:-1], refs[-1]
    feat = pieces[0].shape[1]
    group = group_ref[0]
    for mask, piece in enumerate(pieces):
        first = pl.multiple_of((group ^ mask) * feat, 128)
        out_ref[:, pl.ds(first, feat)] = piece[...]


def unpack(group, pieces):
    tokens, feat = pieces[0].shape
    return pl.pallas_call(
        unpack_kernel,
        in_specs=scalar() + local(len(pieces)),
        out_specs=pl.BlockSpec(memory_space=VMEM),
        out_shape=jax.ShapeDtypeStruct((tokens, len(pieces) * feat), pieces[0].dtype),
        compiler_params=PARAMS,
    )(group, *map(inside, pieces))


def inside(x):
    return pltpu.with_memory_space_constraint(x, pltpu.MemorySpace.VMEM)


def shards(queries, keys, values):
    heads, width = queries.shape[1:]
    devices = lax.axis_size("sp")
    groups = min(GROUPS, heads & -heads, devices // CORES)
    regions = devices // (groups * CORES)
    scale = math.log2(math.e) / math.sqrt(width)
    group = (lax.axis_index("sp") // CORES % groups).astype(jnp.int32).reshape(1)

    def across(piece, mask, step):
        pairs = []
        for i in range(devices):
            region, own, core = i // (groups * CORES), i // CORES % groups, i % CORES
            pairs.append((i, (((region + step) % regions) * groups + (own ^ mask)) * CORES + core))
        return lax.ppermute(piece, "sp", pairs)

    def sibling(piece):
        pairs = [(i, i // CORES * CORES + (i + 1) % CORES) for i in range(devices)]
        return lax.ppermute(piece, "sp", pairs)

    near, far = pack(group, queries, keys, values, groups)
    far_in, near_in, near_all = [], [near[0]], []
    for step in range(1, regions):
        for mask in reversed(range(groups)):
            far_in.append(across(far[mask], mask, step))
    for mask in range(1, groups):
        near_in.append(across(near[mask], mask, 0))
    near_all = near_in + [sibling(far[0])] + [sibling(piece) for piece in near_in[1:]]
    state = attend_first(near_all, groups, scale)
    half = len(far_in) // 2
    early = far_in[:half] + [sibling(piece) for piece in far_in[:half]]
    late = far_in[half:] + [sibling(piece) for piece in far_in[half:]]
    state = attend_middle(state, early, scale)
    results = attend_last(state, late, groups, scale)
    returned = [results[0]] + [across(results[mask], mask, 0) for mask in range(1, groups)]
    return unpack(group, returned)


def solution(mesh):
    spec = P(("dp", "sp"), None, None)
    return jax.shard_map(
        shards,
        mesh=mesh,
        in_specs=(spec, spec, spec),
        out_specs=P(("dp", "sp"), None),
        check_vma=False,
    )
```

```python
import functools
import math

import jax
import jax.numpy as jnp
from jax import lax
from jax.experimental import pallas as pl
from jax.experimental.pallas import tpu as pltpu
from jax.sharding import PartitionSpec as P


CORES = 2
GROUPS = 4

VMEM = pltpu.MemorySpace.VMEM
SMEM = pltpu.MemorySpace.SMEM
PARAMS = pltpu.CompilerParams(vmem_limit_bytes=24 << 20)


def local(count):
    return [pl.BlockSpec(memory_space=VMEM)] * count


def scalar():
    return [pl.BlockSpec(memory_space=SMEM)]


def pack_kernel(group_ref, q_ref, k_ref, v_ref, *refs, groups):
    near, far = refs[:groups], refs[groups : 2 * groups]
    landed, wide, arrived = refs[2 * groups :]
    tokens, heads, width = q_ref.shape
    per_group = heads // groups
    group = group_ref[0]
    copies = []
    for part, ref in enumerate((k_ref, v_ref, q_ref)):
        copies.append(pltpu.make_async_copy(ref, landed.at[part], arrived.at[part]))
        copies[part].start()
    for part in range(3):
        copies[part].wait()
        wide[part] = landed[part].reshape(tokens * heads, width).astype(jnp.float32)
        for mask in range(groups):
            first = (group ^ mask) * per_group
            for head in range(per_group):
                rows = wide[part, pl.ds(first + head, tokens, stride=heads), :].astype(q_ref.dtype)
                near[mask][part, head] = rows
                if part < 2:
                    far[mask][part, head] = rows


def pack(group, queries, keys, values, groups):
    tokens, heads, width = queries.shape
    near = pltpu.VMEM((3, heads // groups, tokens, width), queries.dtype)
    far = pltpu.VMEM((2, heads // groups, tokens, width), queries.dtype)
    outs = pl.pallas_call(
        functools.partial(pack_kernel, groups=groups),
        in_specs=scalar() + [pl.BlockSpec(memory_space=pltpu.MemorySpace.HBM)] * 3,
        out_specs=local(2 * groups),
        out_shape=[near] * groups + [far] * groups,
        scratch_shapes=[
            pltpu.VMEM((3, tokens, heads, width), queries.dtype),
            pltpu.VMEM((3, tokens * heads, width), jnp.float32),
            pltpu.SemaphoreType.DMA((3,)),
        ],
        compiler_params=PARAMS,
    )(group, *(pltpu.with_memory_space_constraint(x, pltpu.MemorySpace.HBM) for x in (queries, keys, values)))
    return outs[:groups], outs[groups:]


def block(head_q, pieces, head, scale):
    head_k = jnp.concatenate([piece[0, head] for piece in pieces])
    head_v = jnp.concatenate([piece[1, head] for piece in pieces])
    scores = lax.dot_general(head_q, head_k, (((1,), (1,)), ((), ())), preferred_element_type=jnp.float32)
    largest = jnp.max(scores, axis=-1, keepdims=True)
    weights = jnp.exp2((scores - largest) * scale)
    total = jnp.sum(weights, axis=-1, keepdims=True)
    summed = jnp.dot(weights.astype(head_v.dtype), head_v, preferred_element_type=jnp.float32)
    return largest, total, summed


def first_kernel(*refs, groups, count, scale):
    pieces, (q_out, largest_out, total_out, summed_out) = refs[:count], refs[count:]
    for head in range(q_out.shape[0]):
        head_q = jnp.concatenate([piece[2, head] for piece in pieces[:groups]])
        q_out[head] = head_q
        largest, total, summed = block(head_q, pieces, head, scale)
        largest_out[head] = largest
        total_out[head] = total
        summed_out[head] = summed


def attend_first(pieces, groups, scale):
    _, per_group, tokens, width = pieces[0].shape
    rows = groups * tokens
    return pl.pallas_call(
        functools.partial(first_kernel, groups=groups, count=len(pieces), scale=scale),
        in_specs=local(len(pieces)),
        out_specs=local(4),
        out_shape=[
            pltpu.VMEM((per_group, rows, width), pieces[0].dtype),
            pltpu.VMEM((per_group, rows, 1), jnp.float32),
            pltpu.VMEM((per_group, rows, 1), jnp.float32),
            pltpu.VMEM((per_group, rows, width), jnp.float32),
        ],
        compiler_params=PARAMS,
    )(*map(inside, pieces))


def merge(refs, pieces, head, scale):
    q_ref, largest_ref, total_ref, summed_ref = refs
    largest, total, summed = block(q_ref[head], pieces, head, scale)
    before = largest_ref[head]
    top = jnp.maximum(largest, before)
    now, then = jnp.exp2((largest - top) * scale), jnp.exp2((before - top) * scale)
    return top, now, then, total * now + total_ref[head] * then, summed, summed_ref[head]


def last_kernel(*refs, count, scale):
    state, pieces, outs = refs[:4], refs[4 : 4 + count], refs[4 + count :]
    per_group, tokens, width = pieces[0].shape[1:]
    for head in range(per_group):
        _, now, then, total, summed, earlier = merge(state, pieces, head, scale)
        inverse = 1.0 / total
        result = summed * (now * inverse) + earlier * (then * inverse)
        result = result.astype(pieces[0].dtype)
        for mask, out in enumerate(outs):
            out[:, head * width : (head + 1) * width] = result[mask * tokens : (mask + 1) * tokens]


def attend_last(state, pieces, groups, scale):
    _, per_group, tokens, width = pieces[0].shape
    out = pltpu.VMEM((tokens, per_group * width), pieces[0].dtype)
    return pl.pallas_call(
        functools.partial(last_kernel, count=len(pieces), scale=scale),
        in_specs=local(4 + len(pieces)),
        out_specs=local(groups),
        out_shape=[out] * groups,
        compiler_params=PARAMS,
    )(*map(inside, state), *map(inside, pieces))


def unpack_kernel(group_ref, *refs):
    pieces, out_ref = refs[:-1], refs[-1]
    feat = pieces[0].shape[1]
    group = group_ref[0]
    for mask, piece in enumerate(pieces):
        first = pl.multiple_of((group ^ mask) * feat, 128)
        out_ref[:, pl.ds(first, feat)] = piece[...]


def unpack(group, pieces):
    tokens, feat = pieces[0].shape
    return pl.pallas_call(
        unpack_kernel,
        in_specs=scalar() + local(len(pieces)),
        out_specs=pl.BlockSpec(memory_space=VMEM),
        out_shape=jax.ShapeDtypeStruct((tokens, len(pieces) * feat), pieces[0].dtype),
        compiler_params=PARAMS,
    )(group, *map(inside, pieces))


def inside(x):
    return pltpu.with_memory_space_constraint(x, pltpu.MemorySpace.VMEM)


def shards(queries, keys, values):
    heads, width = queries.shape[1:]
    devices = lax.axis_size("sp")
    groups = min(GROUPS, heads & -heads, devices // CORES)
    regions = devices // (groups * CORES)
    scale = math.log2(math.e) / math.sqrt(width)
    group = (lax.axis_index("sp") // CORES % groups).astype(jnp.int32).reshape(1)

    def across(piece, mask, step):
        pairs = []
        for i in range(devices):
            region, own, core = i // (groups * CORES), i // CORES % groups, i % CORES
            pairs.append((i, (((region + step) % regions) * groups + (own ^ mask)) * CORES + core))
        return lax.ppermute(piece, "sp", pairs)

    def sibling(piece):
        pairs = [(i, i // CORES * CORES + (i + 1) % CORES) for i in range(devices)]
        return lax.ppermute(piece, "sp", pairs)

    near, far = pack(group, queries, keys, values, groups)
    far_in, far_all, near_in, near_all = [], [], [near[0]], []
    for step in range(1, regions):
        for mask in reversed(range(groups)):
            far_in.append(across(far[mask], mask, step))
    for mask in range(1, groups):
        near_in.append(across(near[mask], mask, 0))
    near_all = near_in + [sibling(far[0])] + [sibling(piece) for piece in near_in[1:]]
    state = attend_first(near_all, groups, scale)
    far_all = far_in + [sibling(piece) for piece in far_in]
    results = attend_last(state, far_all, groups, scale)
    returned = [results[0]] + [across(results[mask], mask, 0) for mask in range(1, groups)]
    return unpack(group, returned)


def solution(mesh):
    spec = P(("dp", "sp"), None, None)
    return jax.shard_map(
        shards,
        mesh=mesh,
        in_specs=(spec, spec, spec),
        out_specs=P(("dp", "sp"), None),
        check_vma=False,
    )
```
